256 devices in a mesh: tm: 16 (over y, z_hi), lat: 4 (over z_lo, core), lon: 4 (over x).
Axes of the slice: x: 4, y: 4, z: 8 (z_hi: 4, z_lo: 2; z = z_hi * 2 + z_lo), core: 2. Of those that a mesh axis runs over, the one named last changes fastest.
Arguments:
- anomaly: bfloat16 [1024, 294912], P('tm', ('lat', 'lon')), may hold values from -40 to 40, as said below
- start_basis: bfloat16 [64, 294912], P(None, ('lat', 'lon')), may hold values from -0.01171875 to 0.01171875
Outputs:
- eof_basis: bfloat16 [64, 294912], P(None, ('lat', 'lon'))
- factor_diag: float32 [64], replicated
The draws below stay inside these ranges and needn't reach their ends.
Inputs may be any that keep to these rules, and one draw needn't show every extreme that they name: `anomaly`: Real-valued anomalies whose magnitude varies between hours, latitude rows and longitude columns.
All inputs are finite; a program needn't handle non-finite values.
Results may differ from the reference program's by a relative error of at most 0.035.
Values may be sent and summed in bfloat16 or wider, within the bound.
No kernel may reach another device: no remote copies, remote signals or barrier semaphores. Data moves between devices by JAX's collectives and lax.ppermute only.
A program may use at most 64 MiB of HBM per device.

```python
import jax
import jax.numpy as jnp
from jax import lax

K = 64
ITERS = 3
HOUR_DEV = 64
NLAT = 384
NLON = 768
HOURS = 1024
POINTS = 294912
N_TM = 16


def draw_anomaly(key, part):
    keys = jax.random.split(jax.random.fold_in(key, 17), 4)
    hour_scale = jnp.exp(jax.random.uniform(keys[0], (HOURS, 1, 1), jnp.float32, jnp.log(0.5), jnp.log(2.0)))
    lat_scale = jnp.exp(jax.random.uniform(keys[1], (1, NLAT, 1), jnp.float32, jnp.log(0.3), jnp.log(3.0)))
    lon_scale = jnp.exp(jax.random.uniform(keys[2], (1, 1, NLON), jnp.float32, jnp.log(0.3), jnp.log(3.0)))
    base = jnp.clip(jax.random.normal(keys[3], (HOURS, NLAT, NLON), jnp.float32), -6.0, 6.0)
    values = 0.25 * hour_scale * lat_scale * lon_scale * base
    values = jnp.clip(values, -40.0, 40.0).reshape(HOURS, NLAT * NLON)
    return values.astype(jnp.bfloat16)


def levels(key, dims, pieces, least, high):
    factor_of = 1.0
    for dim, shards_of in pieces:
        steps = jax.random.uniform(jax.random.fold_in(jax.random.fold_in(key, 6), dim), (shards_of,), jnp.float32, least / len(pieces), high / len(pieces))
        factor_of = factor_of * jnp.repeat(jnp.exp(steps), dims[dim] // shards_of).reshape((-1,) + (1,) * (len(dims) - 1 - dim))
    return factor_of


def scatter_about(own_key, shape, spread, most, shards=(), kind=jnp.bfloat16):
    values = spread * jax.random.normal(own_key, shape, jnp.float32)
    if shards:
        values = values * levels(own_key, shape, shards, -0.22, 0.18)
    return jnp.clip(values, -most, most).astype(kind)


def setup_inputs(seed: int = 0) -> dict:
    key_list = jax.random.split(jax.random.key(seed), 3)
    return {
        "anomaly": draw_anomaly(jax.random.fold_in(key_list[2], 71), 0),
        "start_basis": scatter_about(key_list[1], (K, POINTS), (NLAT * NLON) ** -0.5, 0.01171875, ((1, 16),)),
    }


def lat_weight():
    rows = jnp.arange(NLAT, dtype=jnp.float32)
    latitude = (-90.0 + 180.0 * (rows + 0.5) / NLAT) * (jnp.pi / 180.0)
    return jnp.sqrt(jnp.cos(latitude))

def reference(anomaly, start_basis):
    points = NLAT * NLON
    weight_row = jnp.broadcast_to(lat_weight()[:, None], (NLAT, NLON)).reshape(points)
    field_rows = anomaly
    current = start_basis
    factor = jnp.zeros((K, K), jnp.float32)
    for iteration in range(ITERS):
        scaled = (current.astype(jnp.float32) * weight_row).astype(jnp.bfloat16)
        coeffs = lax.dot_general(field_rows.astype(jnp.float32), scaled.astype(jnp.float32), (((1,), (1,)), ((), ())), preferred_element_type=jnp.float32).astype(jnp.bfloat16)
        total = jnp.zeros((K, points), jnp.float32)
        for block in range(N_TM):
            lower = block * HOUR_DEV
            upper = lower + HOUR_DEV
            block_sum = lax.dot_general(coeffs[lower:upper].astype(jnp.float32), field_rows[lower:upper].astype(jnp.float32), (((0,), (0,)), ((), ())), preferred_element_type=jnp.float32).astype(jnp.bfloat16)
            total = total + block_sum.astype(jnp.float32)
        image = total * weight_row / HOURS
        gram_sum = jnp.dot(image, image.T, precision=lax.Precision.HIGHEST)
        factor = jnp.linalg.cholesky(gram_sum)
        solved = lax.linalg.triangular_solve(factor, image, left_side=True, lower=True)
        current = solved.astype(jnp.bfloat16)
    return (current, jnp.diagonal(factor))
```

```python
import jax
import jax.numpy as jnp
from jax import lax
from jax.sharding import PartitionSpec as P

ITERS = 3
NLAT = 384
NLON = 768
GRID = ("lat", "lon")
EXACT = lax.Precision.HIGHEST


def exchanged(parts, axes):
    return lax.all_to_all(parts, axes, split_axis=0, concat_axis=0, tiled=True)


def from_all(shard, axes):
    count = lax.axis_size(axes)
    return exchanged(jnp.broadcast_to(shard[None], (count, *shard.shape)), axes)


def row_weight(global_point):
    lat_index = global_point // NLON
    latitude = (-90.0 + 180.0 * (lat_index.astype(jnp.float32) + 0.5) / NLAT) * (jnp.pi / 180.0)
    return jnp.sqrt(jnp.cos(latitude))


def sum_everywhere(values):
    count = lax.axis_size(GRID)
    lines, rank = values.shape
    mine = exchanged(values.reshape(count, lines // count, rank), GRID).sum(axis=0)
    mine = from_all(mine, "tm").sum(axis=0)
    return from_all(mine, GRID).reshape(lines, rank)


def lower_inverse(factor):
    unit = jnp.eye(factor.shape[0], dtype=jnp.float32)
    return lax.linalg.triangular_solve(factor, unit, left_side=True, lower=True)


def local(anomaly, start_basis):
    hour_rows, points = anomaly.shape
    rank = start_basis.shape[0]
    groups = lax.axis_size("tm")
    hours = hour_rows * groups
    part = points // groups
    block_start = (lax.axis_index("lat") * lax.axis_size("lon") + lax.axis_index("lon")) * points
    weight_row = row_weight(block_start + jnp.arange(points, dtype=jnp.int32))
    weight_part = lax.dynamic_slice_in_dim(weight_row, lax.axis_index("tm") * part, part)

    parts = jnp.moveaxis(anomaly.reshape(hour_rows, groups, part), 1, 0)
    fields = exchanged(parts, "tm").reshape(hours, part)

    scaled = (start_basis.astype(jnp.float32) * weight_row).astype(jnp.bfloat16)
    first = lax.dot_general(
        anomaly, scaled, (((1,), (1,)), ((), ())), preferred_element_type=jnp.float32
    )
    first = from_all(first, GRID).sum(axis=0).astype(jnp.bfloat16)
    coeffs = from_all(first, "tm").reshape(hours, rank)

    for iteration in range(ITERS):
        image = lax.dot_general(
            coeffs, fields, (((0,), (0,)), ((), ())), preferred_element_type=jnp.float32
        )
        image = image * weight_part / hours
        gram = jnp.dot(image, image.T, precision=EXACT)
        if iteration == ITERS - 1:
            break
        scaled = (image * weight_part).astype(jnp.bfloat16)
        raw = lax.dot_general(
            fields, scaled, (((1,), (1,)), ((), ())), preferred_element_type=jnp.float32
        )
        total = sum_everywhere(jnp.concatenate([raw, gram], axis=0))
        factor = jnp.linalg.cholesky(total[hours:])
        inverse = lower_inverse(factor)
        coeffs = jnp.dot(total[:hours], inverse.T, precision=EXACT).astype(jnp.bfloat16)

    gathered = lax.all_gather(image.astype(jnp.bfloat16), "tm", axis=0, tiled=False)
    gram = from_all(from_all(gram, GRID).sum(axis=0), "tm").sum(axis=0)
    factor = jnp.linalg.cholesky(gram)
    inverse = lower_inverse(factor)
    whole = jnp.moveaxis(gathered, 0, 1).reshape(rank, points)
    current = jnp.dot(inverse, whole.astype(jnp.float32), precision=EXACT)
    return (current.astype(jnp.bfloat16), jnp.diagonal(factor))


def solution(mesh):
    in_specs = (P("tm", ("lat", "lon")), P(None, ("lat", "lon")))
    out_specs = (P(None, ("lat", "lon")), P())
    return jax.shard_map(local, mesh=mesh, in_specs=in_specs, out_specs=out_specs, check_vma=False)
```
